512 devices in a mesh: leaf: 16 (over z), row: 8 (over x, core), top: 4 (over y).
Axes of the slice: x: 4, y: 4, z: 16, core: 2. Of those that a mesh axis runs over, the one named last changes fastest.
Arguments:
- loads: bfloat16 [16, 8, 4, 1, 256, 32], P('leaf', 'row', 'top'), may hold values from -6 to 6
- flux_maps: bfloat16 [16, 8, 4, 640, 256], P('leaf', 'row', 'top'), may hold values from -0.375 to 0.375
- chain_maps: float32 [16, 8, 4, 640, 640], P('leaf', 'row', 'top')
- leaf_maps: bfloat16 [16, 8, 4, 1, 256, 256], P('leaf', 'row', 'top'), may hold values from -0.375 to 0.375
- edge_maps: bfloat16 [16, 8, 4, 1, 256, 640], P('leaf', 'row', 'top'), may hold values from -0.25 to 0.25
- top_maps: bfloat16 [16, 8, 4, 1, 256, 128], P('leaf', 'row', 'top'), may hold values from -0.5 to 0.5
- slot_nodes: int32 [16, 8, 4, 128], P('leaf', 'row', 'top'), may hold values from 0 to 8191
- slot_counts: int32 [16, 8, 4], P('leaf', 'row', 'top'), may hold values from 1 to 128, 320 in all within a row
- top_loads: float32 [8192, 32], P('leaf'), may hold values from -6 to 6
- top_inverse: float32 [8192, 8192], P('top', ('leaf', 'row')), may hold values from -0.0234375 to 0.0234375
Outputs:
- solution: bfloat16 [16, 8, 4, 1, 256, 32], P('leaf', 'row', 'top')
- top_values: float32 [8192, 32], P('top')
The draws below stay inside these ranges and needn't reach their ends.
Inputs may be any that keep to these rules, and one draw needn't show every extreme that they name: `slot_counts`: over the 4 subtrees of one x-y cell (same x and y, all t) the live slots sum to 320, and one of those subtrees has all 128 slots live.
All inputs are finite; a program needn't handle non-finite values. No bound on the sum of `slot_counts` on one device may be relied on, other than what follows from the above.
Results may differ from the reference program's by a relative error of at most 0.0046.
Values sent between devices are 32-bit elements; how exact they have to be, the bound alone decides.
No kernel may reach another device: no remote copies, remote signals or barrier semaphores. Data moves between devices by JAX's collectives and lax.ppermute only.
A program may use at most 64 MiB of HBM per device.

```python
import math
import jax
import jax.numpy as jnp
import numpy as np
from jax import lax

NODES = 256
K = 640
CAP = 128
NRHS = 32
LD = 1
SEP = 8192
SUBTREES_ALONG_X = 16
GY = 8
GT = 4


def draw_chain_maps(key, part):
    random_key_list = jax.random.split(jax.random.fold_in(key, 11), 4)
    share = 0.5
    slow_mask = jax.random.uniform(random_key_list[0], (K,)) < share
    slow_rate = 0.25 ** (1.0 / SUBTREES_ALONG_X)
    jitter = jax.random.uniform(random_key_list[1], (SUBTREES_ALONG_X, GY, GT, K), minval=0.5, maxval=1.0)
    rates = jnp.where(slow_mask, 1.0 - (1.0 - slow_rate) * jitter, 0.6 * jitter)
    explode_position = jax.random.randint(random_key_list[2], (2,), 0, SUBTREES_ALONG_X)
    exploding_rows = jnp.any(jnp.arange(SUBTREES_ALONG_X)[:, None] == explode_position[None, :], axis=1)
    rates = rates * jnp.where(exploding_rows[:, None, None, None] & slow_mask, 0.65, 1.0)
    noise = jax.random.normal(random_key_list[3], (SUBTREES_ALONG_X, GY, GT, K, K), jnp.float32) * (0.2 / K ** 0.5)
    merged = rates[..., None] * (jnp.eye(K, dtype=jnp.float32) + noise)
    return merged.astype(jnp.float32)


def plant(drawn, rng, smallest, largest):
    longest = drawn.shape.index(max(drawn.shape))
    spots = []
    for shift in (0, 1):
        where = [jax.random.randint(jax.random.fold_in(rng, axis), (), 0, length) for axis, length in enumerate(drawn.shape)]
        where[longest] = (where[longest] + shift) % drawn.shape[longest]
        spots.append(tuple(where))
    return drawn.at[spots[0]].set(smallest).at[spots[1]].set(largest)


def block_levels(key, shape, shards, smallest, largest):
    gain = 1.0
    for position, shards_of in shards:
        heights = jax.random.uniform(jax.random.fold_in(jax.random.fold_in(key, 6), position), (shards_of,), jnp.float32, smallest / len(shards), largest / len(shards))
        gain = gain * jnp.repeat(jnp.exp(heights), shape[position] // shards_of).reshape((-1,) + (1,) * (len(shape) - 1 - position))
    return gain


def profile(amount, total, most, slope):
    weights = [(1 << 20) // math.isqrt(standing ** slope) + 1 for standing in range(2, amount + 1)]
    spare, counts = total - most - (amount - 1), [1] * (amount - 1)
    while spare > 0:
        movable = [i for i in range(amount - 1) if counts[i] < most]
        mass, budget = sum([weights[i] for i in movable]), spare
        for i in movable:
            more = min(most - counts[i], max(1, budget * weights[i] // mass), spare)
            counts[i] = counts[i] + more
            spare = spare - more
    return np.array([most] + counts)


def ragged_sizes(stream_key, number_of, total, limit, slope):
    if number_of == 2:
        one = jax.random.randint(stream_key, (), max(1, total - limit), min(limit, total - 1) + 1)
        return jnp.stack([one, total - one])
    tallies = jnp.asarray(profile(number_of, total, limit, slope), jnp.int32)
    pairs = (number_of - 1) // 2
    source_of, receiver = tallies[1:1 + 2 * pairs:2], tallies[2:2 + 2 * pairs:2]
    room = jnp.minimum(source_of - 1, limit - receiver)
    moved = jax.random.randint(jax.random.fold_in(stream_key, 1), (pairs,), 0, 1 << 20) % (room + 1)
    tallies = tallies.at[1:1 + 2 * pairs:2].set(source_of - moved).at[2:2 + 2 * pairs:2].set(receiver + moved)
    return tallies[jax.random.permutation(jax.random.fold_in(stream_key, 2), number_of)]


def centred(stream_key, shape, width, bound, cuts=(), kind=jnp.bfloat16):
    factor_of = block_levels(stream_key, shape, cuts, -0.22, 0.18) if cuts else 1.0
    values = jax.random.normal(stream_key, shape, jnp.float32) * width * factor_of
    return jnp.minimum(jnp.maximum(values, -bound), bound).astype(kind)


def setup_inputs(seed: int = 0) -> dict:
    key_of = jax.random.split(jax.random.key(seed), 11)
    loads = centred(key_of[0], (SUBTREES_ALONG_X, GY, GT, LD, NODES, NRHS), 1.0, 6.0, ((0, 16), (1, 8), (2, 4)))
    flux_maps = centred(key_of[1], (SUBTREES_ALONG_X, GY, GT, K, LD * NODES), (LD * NODES) ** -0.5, 0.375, ((0, 16), (1, 8), (2, 4)))
    chain_maps = draw_chain_maps(jax.random.fold_in(key_of[10], 71), 0)
    leaf_maps = centred(key_of[3], (SUBTREES_ALONG_X, GY, GT, LD, NODES, NODES), NODES ** -0.5, 0.375, ((0, 16), (1, 8), (2, 4)))
    edge_maps = centred(key_of[4], (SUBTREES_ALONG_X, GY, GT, LD, NODES, K), K ** -0.5, 0.25, ((0, 16), (1, 8), (2, 4)))
    top_maps = centred(key_of[5], (SUBTREES_ALONG_X, GY, GT, LD, NODES, CAP), CAP ** -0.5, 0.5, ((0, 16), (1, 8), (2, 4)))
    slot_nodes = plant(jax.random.randint(key_of[6], (SUBTREES_ALONG_X, GY, GT, CAP), 0, SEP), jax.random.fold_in(key_of[6], 1), 0, SEP - 1).astype(jnp.int32)
    slot_counts = jax.vmap(lambda own: ragged_sizes(own, GT, GT * CAP * 5 // 8, CAP, 2))(jax.random.split(key_of[7], SUBTREES_ALONG_X * GY)).reshape((SUBTREES_ALONG_X, GY, GT)).astype(jnp.int32)
    top_loads = centred(key_of[8], (SEP, NRHS), 1.0, 6.0, ((0, 16),), jnp.float32)
    top_inverse = centred(key_of[9], (SEP, SEP), (SEP * (1 + SUBTREES_ALONG_X * GY * GT * CAP // SEP)) ** -0.5, 0.0234375, ((0, 4), (1, 128)), jnp.float32)
    return dict(loads=loads, flux_maps=flux_maps, chain_maps=chain_maps, leaf_maps=leaf_maps, edge_maps=edge_maps, top_maps=top_maps, slot_nodes=slot_nodes, slot_counts=slot_counts, top_loads=top_loads, top_inverse=top_inverse)


def reference(loads, flux_maps, chain_maps, leaf_maps, edge_maps, top_maps, slot_nodes, slot_counts, top_loads, top_inverse):
    flattened = loads.reshape(SUBTREES_ALONG_X, GY, GT, LD * NODES, NRHS).astype(jnp.float32)
    fluxes = jnp.einsum("abckn,abcnr->abckr", flux_maps.astype(jnp.float32), flattened)

    def advance_state(before_state, pair):
        combine_operator, flux_part = pair
        after_state = jnp.einsum("gtkj,gtjr->gtkr", combine_operator, before_state, precision=lax.Precision.HIGHEST) + flux_part
        return after_state, after_state

    start_state = jnp.zeros((GY, GT, K, NRHS), jnp.float32)
    _, states = lax.scan(advance_state, start_state, (chain_maps, fluxes))
    edge_rows = states[:, :, :, :CAP, :]
    is_live = jnp.arange(CAP, dtype=jnp.int32)[None, None, None, :] < slot_counts[..., None]
    chosen_entries = jnp.where(is_live[..., None], edge_rows, jnp.float32(0.0))
    top_sum = jax.ops.segment_sum(chosen_entries.reshape(-1, NRHS), slot_nodes.reshape(-1).astype(jnp.int32), num_segments=SEP)
    top_rhs = top_loads - top_sum
    top_values = jnp.dot(top_inverse, top_rhs, precision=lax.Precision.HIGHEST, preferred_element_type=jnp.float32)
    boundary = jnp.where(is_live[..., None], top_values[slot_nodes.astype(jnp.int32)], jnp.float32(0.0))
    states_low = states.astype(jnp.bfloat16).astype(jnp.float32)
    boundary_low = boundary.astype(jnp.bfloat16).astype(jnp.float32)
    summed = jnp.einsum("abclij,abcljr->abclir", leaf_maps.astype(jnp.float32), loads.astype(jnp.float32))
    summed = summed + jnp.einsum("abclik,abckr->abclir", edge_maps.astype(jnp.float32), states_low)
    summed = summed + jnp.einsum("abclis,abcsr->abclir", top_maps.astype(jnp.float32), boundary_low)
    return summed.astype(jnp.bfloat16), top_values
```

```python
import jax
import jax.numpy as jnp
from jax import lax
from jax.sharding import Mesh
from jax.sharding import PartitionSpec as P


ROW = ("row_0", "row_1")
ROW_TOP = ("row_0", "row_1", "top")
LEAF_ROW = ("leaf", "row_0", "row_1")


def exchanged(pieces, axes):
    return lax.all_to_all(pieces, axes, split_axis=0, concat_axis=0, tiled=True)


def copies_from_all(value, axes):
    return exchanged(jnp.broadcast_to(value, (lax.axis_size(axes), *value.shape)), axes)


def parts_of(value):
    high = lax.reduce_precision(value, 8, 7)
    return high.astype(jnp.bfloat16), (value - high).astype(jnp.bfloat16)


def stacked_parts(value, dim):
    return jnp.concatenate(parts_of(value), dim)


def contract_last(left, right):
    return lax.dot_general(
        left, right, (((1,), (1,)), ((), ())), preferred_element_type=jnp.float32
    )


def mapped(stacked_map, state, flux):
    count, width = state.shape
    product = contract_last(stacked_parts(state, 0), stacked_map)
    return product[:count, :width] + product[count:, :width] + product[:count, width:] + flux


def chain(chain_map, flux):
    planes = lax.axis_size("leaf")
    plane = lax.axis_index("leaf")
    half = planes // 2

    def sent(value, pairs):
        return lax.ppermute(value, "leaf", pairs)

    pairs = [(even, even + 1) for even in range(half, planes, 2)]
    map_before = sent(chain_map, pairs)
    flux_before = sent(flux, pairs)
    own = lax.optimization_barrier(stacked_parts(chain_map, 0))
    state = flux
    for step in range(1, half):
        arrived = sent(state, [(step - 1, step)])
        state = jnp.where(plane == step, mapped(own, arrived, flux), state)
    previous = stacked_parts(map_before, 0)
    for step in range(half + 1, planes, 2):
        arrived = sent(state, [(step - 2, step)])
        advanced = mapped(own, mapped(previous, arrived, flux_before), flux)
        state = jnp.where(plane == step, advanced, state)
    beside = sent(state, [(even - 1, even) for even in range(half, planes, 2)])
    is_even = (plane >= half) & (plane % 2 == 0)
    return jnp.where(is_even, mapped(own, beside, flux), state)


def body(
    loads,
    flux_maps,
    chain_maps,
    leaf_maps,
    edge_maps,
    top_maps,
    slot_nodes,
    slot_counts,
    top_loads,
    top_inverse,
):
    nodes, rhs = loads.shape[4:]
    width = chain_maps.shape[-1]
    slots = slot_nodes.shape[-1]
    leaf_size = lax.axis_size("leaf")
    row_size = lax.axis_size(ROW)
    top_size = lax.axis_size("top")
    block = top_loads.shape[0]
    share, columns = top_inverse.shape
    local_loads = loads.reshape(nodes, rhs)

    flux = lax.dot_general(
        local_loads,
        flux_maps.reshape(width, nodes),
        (((0,), (1,)), ((), ())),
        preferred_element_type=jnp.float32,
    )
    states = chain(chain_maps.reshape(width, width), flux)

    live = lax.iota(jnp.int32, slots) < slot_counts.reshape(())
    ids = jnp.where(live, slot_nodes.reshape(slots), -1)
    id_row = ids.astype(jnp.float32)[None]
    entries = copies_from_all(jnp.concatenate([states[:, :slots], id_row]), "leaf")

    first_node = lax.axis_index("leaf") * block
    entry_ids = entries[:, rhs].astype(jnp.int32).reshape(1, -1) - first_node
    match = (lax.iota(jnp.int32, block)[:, None] == entry_ids).astype(jnp.bfloat16)
    values = jnp.swapaxes(entries[:, :rhs], 0, 1).reshape(rhs, -1)
    dense = contract_last(stacked_parts(values, 0), match)
    dense = (dense[:rhs] + dense[rhs:]).reshape(2, rhs // 2, row_size, columns)
    packed = dense.transpose(2, 1, 0, 3).reshape(row_size, 1, rhs // 2, 2 * columns)
    packed = jnp.broadcast_to(packed, (row_size, top_size, rhs // 2, 2 * columns))
    own_ids = jnp.broadcast_to(id_row, (row_size, top_size, 1, slots))
    pieces = jnp.concatenate([packed, own_ids], 2)
    arrived = exchanged(pieces.reshape(-1, *pieces.shape[2:]), ROW_TOP)

    row = lax.axis_index(ROW)
    top_sum = arrived[:, : rhs // 2].sum(0).reshape(rhs // 2, 2, columns)
    top_sum = top_sum.transpose(1, 0, 2).reshape(rhs, columns)
    cell_ids = lax.dynamic_slice_in_dim(arrived[:, rhs // 2], row * top_size, top_size, 0)
    own_top_loads = lax.dynamic_slice_in_dim(top_loads, row * columns, columns, 0)
    top_rhs = own_top_loads.T - top_sum
    high, low = parts_of(top_rhs)
    inverse = stacked_parts(top_inverse, 1)
    left = jnp.concatenate(
        [jnp.concatenate([high, high], 1), jnp.concatenate([low, jnp.zeros_like(low)], 1)]
    )
    partial = contract_last(left, inverse)
    partial = partial[:rhs] + partial[rhs:]

    group = rhs // row_size
    by_row = exchanged(partial.reshape(row_size, group, share), ROW).sum(0)
    lanes = share // leaf_size
    by_leaf = jnp.swapaxes(by_row.reshape(group, leaf_size, lanes), 0, 1)
    finished = exchanged(by_leaf, "leaf").sum(0)
    band = jnp.swapaxes(copies_from_all(finished, "leaf"), 0, 1).reshape(group, share)
    values = copies_from_all(band, ROW).reshape(rhs, share)

    first_value = lax.axis_index("top") * share
    wanted = cell_ids.astype(jnp.int32).reshape(1, -1) - first_value
    match = (lax.iota(jnp.int32, share)[:, None] == wanted).astype(jnp.bfloat16)
    chosen = jnp.dot(values.astype(jnp.bfloat16), match, preferred_element_type=jnp.float32)
    chosen = jnp.swapaxes(chosen.reshape(rhs, top_size, slots), 0, 1)
    boundary = exchanged(chosen, "top").sum(0)

    summed = jnp.dot(
        leaf_maps.reshape(nodes, nodes), local_loads, preferred_element_type=jnp.float32
    )
    summed = summed + contract_last(
        edge_maps.reshape(nodes, width), states.astype(jnp.bfloat16)
    )
    summed = summed + contract_last(
        top_maps.reshape(nodes, slots), boundary.astype(jnp.bfloat16)
    )
    solution = summed.astype(jnp.bfloat16).reshape(1, 1, 1, 1, nodes, rhs)
    return solution, values.T


def solution(mesh):
    split = Mesh(
        mesh.devices.reshape(mesh.shape["leaf"], -1, 2, mesh.shape["top"]),
        ("leaf", "row_0", "row_1", "top"),
    )
    placed = (
        P("leaf", ROW, "top", None, None, None),
        P("leaf", ROW, "top", None, None),
        P("leaf", ROW, "top", None, None),
        P("leaf", ROW, "top", None, None, None),
        P("leaf", ROW, "top", None, None, None),
        P("leaf", ROW, "top", None, None, None),
        P("leaf", ROW, "top", None),
        P("leaf", ROW, "top"),
        P("leaf", None),
        P("top", LEAF_ROW),
    )

    return jax.shard_map(
        body,
        mesh=split,
        in_specs=placed,
        out_specs=(P("leaf", ROW, "top", None, None, None), P("top", None)),
        check_vma=False,
    )
```
